32 devices in a mesh: expert: 8 (over z, core), hidden: 4 (over y, x).
Axes of the slice: x: 2, y: 2, z: 4, core: 2. Of those that a mesh axis runs over, the one named last changes fastest.
Arguments:
- inputs: bfloat16 [1536, 2880], P('expert', 'hidden'), may hold values from -6 to 6
- out_grad: bfloat16 [1536, 2880], P('expert', 'hidden'), may hold values from -6 to 6
- expert_ids: int32 [1536, 4], P('expert'), may hold values from 0 to 7, all different within a row; in each aligned block of 192 rows (0 to 191, 192 to 383, ...) at most 144 rows name the same one
- route_weight: float32 [1536, 4], P('expert'), may hold values from 0.1 to 1
- w_gate: bfloat16 [8, 2880, 2880], P('expert', 'hidden'), may hold values from -0.109375 to 0.109375
- w_up: bfloat16 [8, 2880, 2880], P('expert', 'hidden'), may hold values from -0.109375 to 0.109375
- w_down: bfloat16 [8, 2880, 2880], P('expert', 'hidden'), may hold values from -0.109375 to 0.109375
Outputs:
- grad_input: bfloat16 [1536, 2880], P('expert', 'hidden')
- grad_route: float32 [1536, 4], P('expert')
- grad_gate: float32 [8, 2880, 2880], P('expert', 'hidden')
- grad_up: float32 [8, 2880, 2880], P('expert', 'hidden')
- grad_down: float32 [8, 2880, 2880], P('expert', 'hidden')
The draws below stay inside these ranges and needn't reach their ends.
Inputs may be any that keep to these rules, and one draw needn't show every extreme that they name: `expert_ids`: each token names 4 different experts. Among the 192 tokens of one index of the expert axis no expert is named more than 144 times, a bound that some block reaches.
All inputs are finite; a program needn't handle non-finite values.
Results may differ from the reference program's by a relative error of at most 0.018.
Values may be sent and summed in bfloat16 or wider, within the bound.
A program may use at most 128 MiB of HBM per device.

```python
import math
import jax
import jax.numpy as jnp
import numpy as np
from jax import lax

D = 2880
FF = 2880
TOP = 4
TOK_DEV = 192
EXPERTS = 8
TOKENS = 1536
CAP = 144
N_EXPERT = 8


def steps_of(rng, extent, split, least, high):
    def one(axis_at, parts):
        heights = jax.random.uniform(jax.random.fold_in(jax.random.fold_in(rng, 6), axis_at), (parts,), jnp.float32, least / len(split), high / len(split))
        return jnp.repeat(jnp.exp(heights), extent[axis_at] // parts).reshape((-1,) + (1,) * (len(extent) - axis_at - 1))

    loudness = one(*split[0])
    for cut in split[1:]:
        loudness = loudness * one(*cut)
    return loudness


def deal_out(stream_key, own, number, rows, amount, top, most, skew):
    sequence = jax.random.permutation(stream_key, amount)
    crowded, common = shares(amount, rows * top, most, skew, True), shares(amount, rows * top, most, skew, False)
    places = jnp.arange(amount)

    def named(tallies, rotation):
        used = int((tallies > 0).sum())
        fixed = max(1, used // 4)
        moved = fixed + (places - fixed + rotation * (used - fixed)) % max(1, amount - fixed)
        return jnp.zeros((amount,), jnp.int32).at[sequence[jnp.where(places < fixed, places, moved)]].set(jnp.asarray(tallies, jnp.int32))

    tallies = jnp.where(number % 4 == 0, named(crowded, number // 4), named(common, number - number // 4 - 1))
    mixed = jax.random.permutation(jax.random.fold_in(own, 3), amount)
    donor, sink = mixed[0:amount // 2 * 2:2], mixed[1:amount // 2 * 2:2]
    room = jnp.minimum(tallies[donor] - 1, most - tallies[sink]) // 2
    room = jnp.where((donor == sequence[0]) | (sink == sequence[0]) | (tallies[sink] == 0), 0, jnp.maximum(room, 0))
    moved = jax.random.randint(jax.random.fold_in(own, 4), (amount // 2,), 0, 1 << 20) % (room + 1)
    tallies = tallies.at[donor].add(-moved).at[sink].add(moved)
    members = jnp.searchsorted(jnp.cumsum(tallies), jnp.arange(rows * top), side="right").astype(jnp.int32)
    grid = members.reshape(top, rows).T
    grid = grid[jax.random.permutation(jax.random.fold_in(own, 1), rows)]
    rotation = jax.random.randint(jax.random.fold_in(own, 2), (rows, 1), 0, top)
    return jnp.take_along_axis(grid, (jnp.arange(top)[None, :] + rotation) % top, axis=1)


def shares(amount, total, limit, lean, full):
    weights = [(1 << 20) // math.isqrt(standing ** lean) + 1 for standing in range(1, amount + 1)]
    largest = limit if full else min(limit, max(-(-total // amount), total * weights[0] // sum(weights)))
    least = 1 if total - largest >= amount - 1 else 0
    holding, spare = [largest] + [least] * (amount - 1), total - largest - least * (amount - 1)
    while spare > 0:
        movable = [i for i in range(1, amount) if holding[i] < largest] or [i for i in range(1, amount) if holding[i] < limit]
        whole, remaining = sum([weights[i] for i in movable]), spare
        for i in movable:
            more = min(limit - holding[i], max(1, remaining * weights[i] // whole), spare)
            holding[i] = holding[i] + more
            spare = spare - more
    return np.array(holding)


def noise(stream_key, extent, deviation, limit, cuts=(), kind=jnp.bfloat16):
    loudness = steps_of(stream_key, extent, cuts, -0.22, 0.18) if cuts else 1.0
    array = jax.random.normal(stream_key, extent, jnp.float32) * deviation * loudness
    return jnp.minimum(jnp.maximum(array, -limit), limit).astype(kind)


def setup_inputs(seed: int = 0) -> dict:
    splits = jax.random.split(jax.random.key(seed), 8)
    inputs = noise(splits[0], (TOKENS, D), 1.0, 6.0, ((0, 8), (1, 4)))
    out_grad = noise(splits[1], (TOKENS, D), 1.0, 6.0, ((0, 8), (1, 4)))
    expert_ids_keys = jax.random.split(jax.random.fold_in(splits[2], 1), TOKENS // TOK_DEV)
    expert_ids_turns = jax.random.permutation(jax.random.fold_in(splits[2], 3), TOKENS // TOK_DEV)
    expert_ids = jax.vmap(lambda own, number: deal_out(jax.random.fold_in(splits[2], 2), own, number, TOK_DEV, EXPERTS, TOP, CAP, 2))(expert_ids_keys, expert_ids_turns).reshape((TOKENS, TOP))
    route_weight = jnp.clip(0.1 + 0.9 * jax.random.uniform(splits[3], (TOKENS, TOP), jnp.float32) ** steps_of(splits[3], (TOKENS, TOP), ((0, 8),), -0.2, 0.2), 0.1, 1.0)
    w_gate = noise(splits[4], (EXPERTS, FF, D), D ** -0.5, 0.109375, ((0, 8), (1, 4)))
    w_up = noise(splits[5], (EXPERTS, FF, D), D ** -0.5, 0.109375, ((0, 8), (1, 4)))
    w_down = noise(splits[6], (EXPERTS, FF, D), FF ** -0.5, 0.109375, ((0, 8), (1, 4)))
    return {"inputs": inputs, "out_grad": out_grad, "expert_ids": expert_ids, "route_weight": route_weight, "w_gate": w_gate, "w_up": w_up, "w_down": w_down}


def reference(inputs, out_grad, expert_ids, route_weight, w_gate, w_up, w_down):
    pairs = TOK_DEV * TOP
    ids = expert_ids.reshape(N_EXPERT, pairs).astype(jnp.int32)
    onehot = (ids[:, :, None] == jnp.arange(EXPERTS, dtype=jnp.int32)[None, None, :]).astype(jnp.int32)
    position = jnp.cumsum(onehot, axis=1) - 1
    slot = jnp.sum(onehot * position, axis=2).astype(jnp.int32)
    source = jnp.arange(N_EXPERT, dtype=jnp.int32)[:, None]
    where = (ids * (N_EXPERT * CAP) + source * CAP + slot).reshape(-1).astype(jnp.int32)
    assign = jnp.arange(N_EXPERT * pairs, dtype=jnp.int32)
    table = jnp.zeros((EXPERTS * N_EXPERT * CAP,), jnp.int32).at[where].set(assign)
    filled = jnp.zeros((EXPERTS * N_EXPERT * CAP,), jnp.int32).at[where].set(1)
    table = table.reshape(EXPERTS, N_EXPERT * CAP)
    filled = filled.reshape(EXPERTS, N_EXPERT * CAP)
    flat_weight = route_weight.reshape(-1)

    def one_expert(carry, pieces):
        grad_acc, route_acc = carry
        rows_idx, used, wg, wu, wd = pieces
        token_idx = (rows_idx // TOP).astype(jnp.int32)
        mask = used.astype(jnp.float32)
        xs = inputs[token_idx] * used.astype(jnp.bfloat16)[:, None]
        dys = out_grad[token_idx] * used.astype(jnp.bfloat16)[:, None]
        weights = flat_weight[rows_idx] * mask
        gate = jnp.dot(xs, wg.T, preferred_element_type=jnp.float32)
        up = jnp.dot(xs, wu.T, preferred_element_type=jnp.float32)
        sig = jax.nn.sigmoid(gate)
        act = gate * sig
        hidden = (act * up).astype(jnp.bfloat16)
        back = jnp.dot(dys, wd.T, preferred_element_type=jnp.float32)
        route_part = jnp.sum(hidden.astype(jnp.float32) * back, axis=1)
        grad_hidden = weights[:, None] * back
        scaled = (weights[:, None] * dys.astype(jnp.float32)).astype(jnp.bfloat16)
        gdown = jnp.dot(hidden.T, scaled, preferred_element_type=jnp.float32)
        d_gate = (grad_hidden * up * sig * (1.0 + gate * (1.0 - sig))).astype(jnp.bfloat16)
        d_up = (grad_hidden * act).astype(jnp.bfloat16)
        ggate = jnp.dot(d_gate.T, xs, preferred_element_type=jnp.float32)
        gup = jnp.dot(d_up.T, xs, preferred_element_type=jnp.float32)
        row_grad = jnp.dot(d_gate, wg, preferred_element_type=jnp.float32) + jnp.dot(d_up, wu, preferred_element_type=jnp.float32)
        grad_acc = grad_acc.at[token_idx].add(row_grad * mask[:, None])
        route_acc = route_acc.at[rows_idx].add(route_part * mask)
        return (grad_acc, route_acc), (ggate, gup, gdown)

    start = (jnp.zeros((TOKENS, D), jnp.float32), jnp.zeros((TOKENS * TOP,), jnp.float32))
    (grad_acc, route_acc), (grad_gate, grad_up, grad_down) = lax.scan(one_expert, start, (table, filled, w_gate, w_up, w_down))
    return grad_acc.astype(jnp.bfloat16), route_acc.reshape(TOKENS, TOP), grad_gate, grad_up, grad_down
```

```python
import functools

import jax
import jax.numpy as jnp
from jax import lax
from jax.experimental import pallas as pl
from jax.experimental.pallas import tpu as pltpu
from jax.sharding import PartitionSpec as P


def slot_tables(expert_ids, experts, capacity):
    count, top = expert_ids.shape
    flat = expert_ids.reshape(-1)
    onehot = (flat[:, None] == jnp.arange(experts, dtype=jnp.int32)[None, :]).astype(jnp.int32)
    position = jnp.cumsum(onehot, axis=0) - 1
    slot = jnp.sum(onehot * position, axis=1)
    dest = flat * capacity + slot
    table = (
        jnp.zeros((experts * capacity,), jnp.int32)
        .at[dest]
        .set(jnp.arange(count * top, dtype=jnp.int32))
    )
    filled = jnp.zeros((experts * capacity,), jnp.int32).at[dest].set(1)
    return (dest, table, filled)


def pack_rows(values, table, filled, top, experts, capacity):
    picked = values[table // top] * filled.astype(values.dtype)[:, None]
    return picked.reshape(experts, capacity, values.shape[1])


def to_local(buffer, n_groups, local_count):
    rest = buffer.shape[2:]
    shaped = buffer.reshape((n_groups, local_count, buffer.shape[1]) + rest)
    return jnp.swapaxes(shaped, 0, 1).reshape((local_count, n_groups * buffer.shape[1]) + rest)


def from_local(buffer, n_groups, capacity):
    local_count = buffer.shape[0]
    rest = buffer.shape[2:]
    shaped = buffer.reshape((local_count, n_groups, capacity) + rest)
    return jnp.swapaxes(shaped, 0, 1).reshape((n_groups * local_count, capacity) + rest)


def plain_device(inputs, out_grad, expert_ids, route_weight, w_gate, w_up, w_down):
    n_groups = lax.axis_size("expert")
    local_count = w_gate.shape[0]
    experts = local_count * n_groups
    tok_count, top = expert_ids.shape
    capacity = 3 * top * tok_count // (2 * experts)
    dest, table, filled = slot_tables(expert_ids, experts, capacity)
    send_weight = (route_weight.reshape(-1)[table] * filled.astype(jnp.float32)).reshape(
        experts, capacity
    )
    send_x = pack_rows(inputs, table, filled, top, experts, capacity)
    send_dy = pack_rows(out_grad, table, filled, top, experts, capacity)
    got_x, got_dy, got_weight = (
        lax.all_to_all(send_x, "expert", split_axis=0, concat_axis=0, tiled=True),
        lax.all_to_all(send_dy, "expert", split_axis=0, concat_axis=0, tiled=True),
        lax.all_to_all(
            send_weight.astype(jnp.bfloat16), "expert", split_axis=0, concat_axis=0, tiled=True
        ).astype(send_weight.dtype),
    )
    rows_x, rows_dy = (
        lax.all_gather(got_x, "hidden", axis=2, tiled=True),
        lax.all_gather(got_dy, "hidden", axis=2, tiled=True),
    )
    xs = to_local(rows_x, n_groups, local_count)
    dys = to_local(rows_dy, n_groups, local_count)
    weights = to_local(got_weight, n_groups, local_count)
    gate = jnp.einsum("esd,efd->esf", xs, w_gate, preferred_element_type=jnp.float32)
    up = jnp.einsum("esd,efd->esf", xs, w_up, preferred_element_type=jnp.float32)
    sig = jax.nn.sigmoid(gate)
    act = gate * sig
    hidden = (act * up).astype(jnp.bfloat16)
    back = jnp.einsum("esd,efd->esf", dys, w_down, preferred_element_type=jnp.float32)
    route_part = jnp.sum(hidden.astype(jnp.float32) * back, axis=2)
    grad_hidden = weights[:, :, None] * back
    scaled = (weights[:, :, None] * dys.astype(jnp.float32)).astype(jnp.bfloat16)
    grad_down = jnp.einsum("esf,esd->efd", hidden, scaled, preferred_element_type=jnp.float32)
    d_gate = (grad_hidden * up * sig * (1.0 + gate * (1.0 - sig))).astype(jnp.bfloat16)
    d_up = (grad_hidden * act).astype(jnp.bfloat16)
    grad_gate = jnp.einsum("esf,esd->efd", d_gate, xs, preferred_element_type=jnp.float32)
    grad_up = jnp.einsum("esf,esd->efd", d_up, xs, preferred_element_type=jnp.float32)
    partial_value = jnp.einsum("esf,efd->esd", d_gate, w_gate, preferred_element_type=jnp.float32)
    partial_value = partial_value + jnp.einsum(
        "esf,efd->esd", d_up, w_up, preferred_element_type=jnp.float32
    )
    route_total = lax.psum(route_part, "hidden")
    route_back = from_local(route_total, n_groups, capacity)
    summed = lax.psum_scatter(
        partial_value.astype(jnp.bfloat16), "hidden", scatter_dimension=2, tiled=True
    ).astype(jnp.float32)
    back_rows, back_route = (
        lax.all_to_all(
            from_local(summed, n_groups, capacity).astype(jnp.bfloat16),
            "expert",
            split_axis=0,
            concat_axis=0,
            tiled=True,
        ).astype(jnp.float32),
        lax.all_to_all(
            route_back.astype(jnp.bfloat16), "expert", split_axis=0, concat_axis=0, tiled=True
        ).astype(route_back.dtype),
    )
    per_pair = back_rows.reshape(experts * capacity, back_rows.shape[2])[dest]
    grad_input = jnp.sum(per_pair.reshape(tok_count, top, per_pair.shape[1]), axis=1).astype(
        jnp.bfloat16
    )
    grad_route = back_route.reshape(-1)[dest].reshape(tok_count, top)
    return (grad_input, grad_route, grad_gate, grad_up, grad_down)


MESH = pl.DeviceIdType.MESH
F32 = jnp.float32
BF16 = jnp.bfloat16


def places():
    e, h = lax.axis_index("expert"), lax.axis_index("hidden")
    core, z = e % 2, e // 2
    x, y = h % 2, h // 2
    across_x = (e, y * 2 + (1 - x))
    across_y = (e, (1 - y) * 2 + x)
    sibling = (z * 2 + (1 - core), h)
    return e, h, z, core, x, y, across_x, across_y, sibling


def flip(z, j):
    low = z % 2 + j % 2 - 2 * (z % 2) * (j % 2)
    high = z // 2 + j // 2 - 2 * (z // 2) * (j // 2)
    return low + 2 * high


def greet(n_expert, e, h, across_x, across_y):
    barrier = pltpu.get_barrier_semaphore()
    peers = [((e + i) % n_expert, h) for i in range(1, n_expert)] + [across_x, across_y]
    for peer in peers:
        pl.semaphore_signal(barrier, inc=1, device_id=peer, device_id_type=MESH)
    pl.semaphore_wait(barrier, len(peers))


def send(src, dst, send_sem, recv_sem, device):
    return pltpu.make_async_remote_copy(
        src_ref=src, dst_ref=dst, send_sem=send_sem, recv_sem=recv_sem,
        device_id=device, device_id_type=MESH,
    )


def routed(meta, e):
    top = meta.shape[0] // 2
    hits = (meta[:top] == e.astype(F32)).astype(F32)
    return hits, jnp.sum(hits * meta[top:], axis=0, keepdims=True)


def diagonal(count):
    return (
        lax.broadcasted_iota(jnp.int32, (count, count), 0)
        == lax.broadcasted_iota(jnp.int32, (count, count), 1)
    ).astype(F32)


def fused_kernel(
    n_expert, x_ref, dy_ref, meta_ref, wg_hbm, wu_hbm, wd_hbm,
    w, grad_out, route_out,
    g, gm, d, tok, got_a, got_bx, got_by, got_c, got_d,
    route, route_x, route_s, route_y, route_t, route_z,
    own_sem, zs, zr, xsem, xr, ysem, yr, ds, dr, ss, sr, ms, mr, w_sem,
    sa, ra, sbx, rbx, sby, rby, sc, rc, sd, rd, sroute, rroute, srx, rrx,
):
    nz = n_expert // 2
    last = nz - 1
    count, width = x_ref.shape
    half = count // 2
    shares = g.shape[1]
    e, h, z, core, x, y, across_x, across_y, sibling = places()
    hx, hy, hd = across_x[1], across_y[1], (1 - y) * 2 + (1 - x)
    load = [
        pltpu.make_async_copy(src, w.at[i], w_sem.at[i])
        for i, src in enumerate((wg_hbm, wu_hbm, wd_hbm))
    ]
    for copy in load:
        copy.start()
    greet(n_expert, e, h, across_x, across_y)
    full = (x_ref, dy_ref)

    def block(t, b, share, start=0, size=count):
        return g.at[t, share, pl.ds(pl.multiple_of(b * count + start, 32), size)]

    own = [pltpu.make_async_copy(full[t], block(t, e, h), own_sem.at[t]) for t in range(2)]
    own.append(pltpu.make_async_copy(meta_ref, gm.at[e], own_sem.at[2]))

    def arrived(slot, send_sem, recv_sem, device):
        send(slot, slot, send_sem, recv_sem, device).wait_recv()

    def meta_to(i):
        return send(meta_ref, gm.at[e], ms.at[i], mr.at[i], ((e + n_expert - i) % n_expert, h))

    def column(j):
        return flip(z, j) * 2 + core

    def z_send(t, i):
        return send(full[t], block(t, e, h), zs.at[t, i], zr.at[t, i], (column(i), h))

    def first_sends(t, j, src):
        slot = block(t, column(j), h)
        src = slot if src is None else src
        return [
            send(src, slot, xsem.at[t, j], xr.at[t, j], across_x),
            send(src, slot, ysem.at[t, j], yr.at[t, j], across_y),
            send(src, slot, ss.at[t, j, 0], sr.at[t, j, 0], sibling),
        ]

    def second_sends(t, j, side):
        share, to = ((hx, across_y), (hy, across_x))[side]
        slot = block(t, column(j), share)
        part = block(t, column(j), share, side * half, half)
        return [
            send(part, part, ds.at[t, j, side], dr.at[t, j, side], to),
            send(slot, slot, ss.at[t, j, 1 + side], sr.at[t, j, 1 + side], sibling),
        ]

    def third_sends(t, j):
        slot = block(t, column(j), hd)
        return [send(slot, slot, ss.at[t, j, 3], sr.at[t, j, 3], sibling)]

    def start(copies):
        for copy in copies:
            copy.start()

    def sent(copies):
        for copy in copies:
            copy.wait_send()

    def first(t, j):
        arrived(block(t, column(j), h), zs.at[t, j], zr.at[t, j], across_x)
        start(first_sends(t, j, None))

    def second(t, j):
        arrived(block(t, column(j), hx), xsem.at[t, j], xr.at[t, j], across_x)
        start(second_sends(t, j, 0))
        arrived(block(t, column(j), hy), ysem.at[t, j], yr.at[t, j], across_y)
        start(second_sends(t, j, 1))

    def third(t, j):
        for k in range(2):
            arrived(block(t, column(j), hd, k * half, half), ds.at[t, j, k], dr.at[t, j, k], across_y)
        start(third_sends(t, j))

    def from_sibling(t, j):
        b = flip(z, j) * 2 + (1 - core)
        for k, part in enumerate((h, hx, hy, hd)):
            arrived(block(t, b, part), ss.at[t, j, k], sr.at[t, j, k], sibling)

    start(first_sends(0, 0, x_ref))
    start([meta_to(i) for i in range(1, n_expert)])
    for t in range(2):
        z_send(t, 1).start()
    start(first_sends(1, 0, dy_ref))
    start(own)
    second(0, 0)
    first(0, 1)
    z_send(0, 2).start()
    second(1, 0)
    first(1, 1)
    z_send(1, 2).start()
    for i in range(3, nz):
        for t in range(2):
            z_send(t, i).start()
    third(0, 0)
    for copy in load + own:
        copy.wait()
    for i in range(1, n_expert):
        arrived(gm.at[(e + i) % n_expert], ms.at[i], mr.at[i], sibling)

    turned = (((1,), (1,)), ((), ()))
    low, high = pl.ds(0, half), pl.ds(half, half)

    def add(a, b):
        return (a.astype(F32) + b.astype(F32)).astype(BF16)

    def a_send(j):
        return send(tok.at[1 - core], got_a.at[j], sa.at[j], ra.at[j], sibling)

    def b_sends(j):
        return [
            send(got_a.at[j, k * 2 + (1 - x), low], got_bx.at[j, k], sbx.at[j, k], rbx.at[j, k], across_x)
            for k in range(2)
        ] + [
            send(got_a.at[j, (1 - y) * 2 + k, high], got_by.at[j, k], sby.at[j, k], rby.at[j, k], across_y)
            for k in range(2)
        ]

    def c_sends(j):
        return [
            send(got_bx.at[j, 1 - y], got_c.at[j, low], sc.at[j, 0], rc.at[j, 0], across_y),
            send(got_by.at[j, 1 - x], got_c.at[j, high], sc.at[j, 1], rc.at[j, 1], across_x),
        ]

    def d_send(j):
        return send(got_c.at[j], got_d.at[j], sd.at[j], rd.at[j], (column(j), h))

    def fold(j):
        a_send(j).wait()
        for s in range(shares):
            got_a[j, s] = add(tok[core, s], got_a[j, s])

    def stage_b(j):
        start(b_sends(j))

    def stage_c(j):
        copies = b_sends(j)
        for k in range(2):
            copies[k].wait_recv()
            got_bx[j, k] = add(got_a[j, k * 2 + x, low], got_bx[j, k])
            copies[2 + k].wait_recv()
            got_by[j, k] = add(got_a[j, y * 2 + k, high], got_by[j, k])
        start(c_sends(j))

    def stage_d(j):
        for copy in c_sends(j):
            copy.wait_recv()
        got_c[j, low] = add(got_bx[j, y], got_c[j, low])
        got_c[j, high] = add(got_by[j, x], got_c[j, high])
        if j:
            d_send(j).start()

    rx = send(route, route_x, srx.at[0], rrx.at[0], across_x)
    ry = send(route_s, route_y, srx.at[1], rrx.at[1], across_y)
    routes = [
        send(route_t.at[(e + i) % n_expert], route_z.at[i], sroute.at[i], rroute.at[i], ((e + i) % n_expert, h))
        for i in range(1, n_expert)
    ]

    def at_share(s):
        return pl.ds(s * width, width)

    def project(t, rows, m):
        total = None
        for s in range(shares):
            part = lax.dot_general(
                g[t, s, rows], w[m, :, at_share(s)], turned, preferred_element_type=F32
            )
            total = part if total is None else total + part
        return total

    eye = diagonal(count)

    def step(j, carry):
        more, further, final = j + 1 < nz, j + 2 < nz, j == last
        plane = flip(z, j)
        rows = pl.ds(pl.multiple_of(plane * (2 * count), 64), 2 * count)
        from_sibling(0, j)

        @pl.when(more)
        def _():
            second(0, j + 1)

        @pl.when(final)
        def _():
            for i in range(1, last - 1):
                stage_b(i)

        gate = project(0, rows, 0)
        up = project(0, rows, 1)

        @pl.when(further)
        def _():
            first(0, j + 2)

        @pl.when(j > 0)
        def _():
            fold(j - 1)

        @pl.when(final)
        def _():
            stage_b(last - 1)

        third(1, j)
        from_sibling(1, j)
        back = project(1, rows, 2)
        hits, weights = [], []
        for c in range(2):
            hit, row = routed(gm[plane * 2 + c], e)
            hits.append(hit)
            weights.append(jnp.sum(eye * row, axis=1, keepdims=True))
        weight = jnp.concatenate(weights, axis=0)
        sig = jax.nn.sigmoid(gate)
        act = gate * sig
        hidden = act * up
        d[2, rows] = (weight * hidden).astype(BF16)
        hidden = hidden.astype(BF16)
        parted = jnp.sum(hidden.astype(F32) * back, axis=1, keepdims=True)
        grad_hidden = weight * back
        d[0, rows] = (grad_hidden * up * sig * (1.0 + gate * (1.0 - sig))).astype(BF16)
        d[1, rows] = (grad_hidden * act).astype(BF16)
        for c in range(2):
            per_token = jnp.sum(eye * parted[c * count : (c + 1) * count], axis=0, keepdims=True)
            top = hits[c].shape[0]
            route[plane * 2 + c, :top] = hits[c] * per_token
            route[plane * 2 + c, top:] = jnp.zeros_like(hits[c])

        @pl.when(more)
        def _():
            second(1, j + 1)

        @pl.when(further)
        def _():
            first(1, j + 2)

        @pl.when(more)
        def _():
            third(0, j + 1)

        @pl.when(final)
        def _():
            rx.start()
            for i in range(1, last - 1):
                stage_c(i)

        for s in range(shares):
            row_grad = (
                jnp.dot(d[0, rows], w[0, :, at_share(s)], preferred_element_type=F32)
                + jnp.dot(d[1, rows], w[1, :, at_share(s)], preferred_element_type=F32)
            ).astype(BF16)
            for c in range(2):
                tok[c, s] = row_grad[c * count : (c + 1) * count]
        a_send(j).start()
        return carry

    lax.fori_loop(0, nz, step, 0)

    def route_on():
        rx.wait_recv()
        route_s[...] = route[...] + route_x[...]
        ry.start()

    def route_out_to_owners():
        ry.wait_recv()
        route_t[...] = route_s[...] + route_y[...]
        start(routes)

    def tail_one():
        route_on()
        for i in range(1, last - 1):
            stage_d(i)
        stage_c(last - 1)
        fold(last)
        stage_b(last)
        stage_b(0)

    events = {
        (0, 0): tail_one,
        (0, 2): route_out_to_owners,
        (0, 3): lambda: stage_d(last - 1),
        (1, 1): lambda: stage_c(last),
        (1, 3): lambda: stage_d(last),
        (2, 1): lambda: stage_c(0),
    }

    def outer(m, carry):
        for s in range(shares):
            w[m, :, at_share(s)] = lax.dot_general(
                d[m], g[m // 2, s], (((0,), (0,)), ((), ())), preferred_element_type=F32
            ).astype(BF16)
            for (at_m, at_s), event in events.items():
                if at_s == s:
                    pl.when(m == at_m)(event)
        return carry

    lax.fori_loop(0, 3, outer, 0)
    stage_d(0)
    total = route_t[e]
    for i in range(1, n_expert):
        routes[i - 1].wait_recv()
        total = total + route_z[i]
    route_out[...] = total
    total = got_c[0].astype(F32)
    for j in range(1, nz):
        d_send(j).wait_recv()
        total = total + got_d[j].astype(F32)
    grad_out[...] = total.astype(BF16)
    sent([rx, ry] + routes + [d_send(j) for j in range(1, nz)])
    for j in range(nz):
        sent(b_sends(j) + c_sends(j))
    for i in range(1, n_expert):
        meta_to(i).wait_send()
    for t in range(2):
        for j in range(nz):
            if j:
                z_send(t, j).wait_send()
            sent(first_sends(t, j, full[t] if j == 0 else None))
            sent(second_sends(t, j, 0) + second_sends(t, j, 1) + third_sends(t, j))


def gather_and_expert(x, dy, meta, w_gate, w_up, w_down, n_expert):
    nz = n_expert // 2
    count, width = x.shape
    hidden, depth = w_gate.shape
    total = n_expert * count
    half = count // 2
    dma = pltpu.SemaphoreType.DMA
    vmem = pl.BlockSpec(memory_space=pltpu.VMEM)
    hbm = pl.BlockSpec(memory_space=pl.ANY)

    def room(*shape):
        return pltpu.VMEM(shape, BF16)

    return pl.pallas_call(
        functools.partial(fused_kernel, n_expert),
        out_shape=(
            jax.ShapeDtypeStruct((3, hidden, depth), BF16),
            jax.ShapeDtypeStruct((count, width), BF16),
            jax.ShapeDtypeStruct(meta.shape, F32),
        ),
        in_specs=[vmem] * 3 + [hbm] * 3,
        out_specs=[vmem] * 3,
        scratch_shapes=[
            room(2, 4, total, width),
            pltpu.VMEM((n_expert,) + meta.shape, F32),
            room(3, total, hidden),
            room(2, 4, count, width),
            room(nz, 4, count, width),
            room(nz, 2, half, width),
            room(nz, 2, half, width),
            room(nz, count, width),
            room(nz, count, width),
        ]
        + [pltpu.VMEM((n_expert,) + meta.shape, F32)] * 6
        + [dma((3,))]
        + [dma((2, nz))] * 6
        + [dma((2, nz, 2))] * 2
        + [dma((2, nz, 4))] * 2
        + [dma((n_expert,))] * 2
        + [dma((3,))]
        + [dma((nz,))] * 2
        + [dma((nz, 2))] * 6
        + [dma((nz,))] * 2
        + [dma((n_expert,))] * 2
        + [dma((2,))] * 2,
        compiler_params=pltpu.CompilerParams(
            collective_id=0, has_side_effects=True, vmem_limit_bytes=63 * 1024 * 1024
        ),
    )(x, dy, meta, w_gate, w_up, w_down)


def paired_device(inputs, out_grad, expert_ids, route_weight, w_gate, w_up, w_down):
    top = expert_ids.shape[1]
    meta = jnp.concatenate([expert_ids.astype(F32).T, route_weight.T], axis=0)
    grads, grad_input, grad_route = gather_and_expert(
        inputs, out_grad, meta, w_gate[0], w_up[0], w_down[0], lax.axis_size("expert")
    )
    wide = [grads[i].astype(F32)[None] for i in range(3)]
    return (grad_input, grad_route[:top].T, *wide)


def solution(mesh):
    placed = (
        P("expert", "hidden"),
        P("expert", "hidden"),
        P("expert", None),
        P("expert", None),
        P("expert", "hidden", None),
        P("expert", "hidden", None),
        P("expert", "hidden", None),
    )
    return jax.shard_map(
        paired_device
        if mesh.shape["hidden"] == 4 and mesh.shape["expert"] == 8
        else plain_device,
        mesh=mesh,
        in_specs=placed,
        out_specs=(
            P("expert", "hidden"),
            P("expert", None),
            P("expert", "hidden", None),
            P("expert", "hidden", None),
            P("expert", "hidden", None),
        ),
        check_vma=False,
    )
```

```python
import functools

import jax
import jax.numpy as jnp
from jax import lax
from jax.experimental import pallas as pl
from jax.experimental.pallas import tpu as pltpu
from jax.sharding import PartitionSpec as P


def slot_tables(expert_ids, experts, capacity):
    count, top = expert_ids.shape
    flat = expert_ids.reshape(-1)
    onehot = (flat[:, None] == jnp.arange(experts, dtype=jnp.int32)[None, :]).astype(jnp.int32)
    position = jnp.cumsum(onehot, axis=0) - 1
    slot = jnp.sum(onehot * position, axis=1)
    dest = flat * capacity + slot
    table = (
        jnp.zeros((experts * capacity,), jnp.int32)
        .at[dest]
        .set(jnp.arange(count * top, dtype=jnp.int32))
    )
    filled = jnp.zeros((experts * capacity,), jnp.int32).at[dest].set(1)
    return (dest, table, filled)


def pack_rows(values, table, filled, top, experts, capacity):
    picked = values[table // top] * filled.astype(values.dtype)[:, None]
    return picked.reshape(experts, capacity, values.shape[1])


def to_local(buffer, n_groups, local_count):
    rest = buffer.shape[2:]
    shaped = buffer.reshape((n_groups, local_count, buffer.shape[1]) + rest)
    return jnp.swapaxes(shaped, 0, 1).reshape((local_count, n_groups * buffer.shape[1]) + rest)


def from_local(buffer, n_groups, capacity):
    local_count = buffer.shape[0]
    rest = buffer.shape[2:]
    shaped = buffer.reshape((local_count, n_groups, capacity) + rest)
    return jnp.swapaxes(shaped, 0, 1).reshape((n_groups * local_count, capacity) + rest)


def plain_device(inputs, out_grad, expert_ids, route_weight, w_gate, w_up, w_down):
    n_groups = lax.axis_size("expert")
    local_count = w_gate.shape[0]
    experts = local_count * n_groups
    tok_count, top = expert_ids.shape
    capacity = 3 * top * tok_count // (2 * experts)
    dest, table, filled = slot_tables(expert_ids, experts, capacity)
    send_weight = (route_weight.reshape(-1)[table] * filled.astype(jnp.float32)).reshape(
        experts, capacity
    )
    send_x = pack_rows(inputs, table, filled, top, experts, capacity)
    send_dy = pack_rows(out_grad, table, filled, top, experts, capacity)
    got_x, got_dy, got_weight = (
        lax.all_to_all(send_x, "expert", split_axis=0, concat_axis=0, tiled=True),
        lax.all_to_all(send_dy, "expert", split_axis=0, concat_axis=0, tiled=True),
        lax.all_to_all(
            send_weight.astype(jnp.bfloat16), "expert", split_axis=0, concat_axis=0, tiled=True
        ).astype(send_weight.dtype),
    )
    rows_x, rows_dy = (
        lax.all_gather(got_x, "hidden", axis=2, tiled=True),
        lax.all_gather(got_dy, "hidden", axis=2, tiled=True),
    )
    xs = to_local(rows_x, n_groups, local_count)
    dys = to_local(rows_dy, n_groups, local_count)
    weights = to_local(got_weight, n_groups, local_count)
    gate = jnp.einsum("esd,efd->esf", xs, w_gate, preferred_element_type=jnp.float32)
    up = jnp.einsum("esd,efd->esf", xs, w_up, preferred_element_type=jnp.float32)
    sig = jax.nn.sigmoid(gate)
    act = gate * sig
    hidden = (act * up).astype(jnp.bfloat16)
    back = jnp.einsum("esd,efd->esf", dys, w_down, preferred_element_type=jnp.float32)
    route_part = jnp.sum(hidden.astype(jnp.float32) * back, axis=2)
    grad_hidden = weights[:, :, None] * back
    scaled = (weights[:, :, None] * dys.astype(jnp.float32)).astype(jnp.bfloat16)
    grad_down = jnp.einsum("esf,esd->efd", hidden, scaled, preferred_element_type=jnp.float32)
    d_gate = (grad_hidden * up * sig * (1.0 + gate * (1.0 - sig))).astype(jnp.bfloat16)
    d_up = (grad_hidden * act).astype(jnp.bfloat16)
    grad_gate = jnp.einsum("esf,esd->efd", d_gate, xs, preferred_element_type=jnp.float32)
    grad_up = jnp.einsum("esf,esd->efd", d_up, xs, preferred_element_type=jnp.float32)
    partial_value = jnp.einsum("esf,efd->esd", d_gate, w_gate, preferred_element_type=jnp.float32)
    partial_value = partial_value + jnp.einsum(
        "esf,efd->esd", d_up, w_up, preferred_element_type=jnp.float32
    )
    route_total = lax.psum(route_part, "hidden")
    route_back = from_local(route_total, n_groups, capacity)
    summed = lax.psum_scatter(
        partial_value.astype(jnp.bfloat16), "hidden", scatter_dimension=2, tiled=True
    ).astype(jnp.float32)
    back_rows, back_route = (
        lax.all_to_all(
            from_local(summed, n_groups, capacity).astype(jnp.bfloat16),
            "expert",
            split_axis=0,
            concat_axis=0,
            tiled=True,
        ).astype(jnp.float32),
        lax.all_to_all(
            route_back.astype(jnp.bfloat16), "expert", split_axis=0, concat_axis=0, tiled=True
        ).astype(route_back.dtype),
    )
    per_pair = back_rows.reshape(experts * capacity, back_rows.shape[2])[dest]
    grad_input = jnp.sum(per_pair.reshape(tok_count, top, per_pair.shape[1]), axis=1).astype(
        jnp.bfloat16
    )
    grad_route = back_route.reshape(-1)[dest].reshape(tok_count, top)
    return (grad_input, grad_route, grad_gate, grad_up, grad_down)


MESH = pl.DeviceIdType.MESH
F32 = jnp.float32
BF16 = jnp.bfloat16


def places():
    e, h = lax.axis_index("expert"), lax.axis_index("hidden")
    core, z = e % 2, e // 2
    x, y = h % 2, h // 2
    across_x = (e, y * 2 + (1 - x))
    across_y = (e, (1 - y) * 2 + x)
    sibling = (z * 2 + (1 - core), h)
    return e, h, z, core, x, y, across_x, across_y, sibling


def flip(z, j):
    low = z % 2 + j % 2 - 2 * (z % 2) * (j % 2)
    high = z // 2 + j // 2 - 2 * (z // 2) * (j // 2)
    return low + 2 * high


def greet(n_expert, e, h, across_x, across_y):
    barrier = pltpu.get_barrier_semaphore()
    peers = [((e + i) % n_expert, h) for i in range(1, n_expert)] + [across_x, across_y]
    for peer in peers:
        pl.semaphore_signal(barrier, inc=1, device_id=peer, device_id_type=MESH)
    pl.semaphore_wait(barrier, len(peers))


def send(src, dst, send_sem, recv_sem, device):
    return pltpu.make_async_remote_copy(
        src_ref=src, dst_ref=dst, send_sem=send_sem, recv_sem=recv_sem,
        device_id=device, device_id_type=MESH,
    )


def routed(meta, e):
    top = meta.shape[0] // 2
    hits = (meta[:top] == e.astype(F32)).astype(F32)
    return hits, jnp.sum(hits * meta[top:], axis=0, keepdims=True)


def diagonal(count):
    return (
        lax.broadcasted_iota(jnp.int32, (count, count), 0)
        == lax.broadcasted_iota(jnp.int32, (count, count), 1)
    ).astype(F32)


def fused_kernel(
    n_expert, x_ref, dy_ref, ids_ref, rw_ref, wg_hbm, wu_hbm, wd_hbm,
    w, grad_out, route_out,
    g, meta_ref, gm, d, tok, got_a, got_bx, got_by, got_c, got_d,
    route, route_x, route_s, route_y, route_t, route_z,
    own_sem, zs, zr, xsem, xr, ysem, yr, ds, dr, ss, sr, ms, mr, w_sem,
    sa, ra, sbx, rbx, sby, rby, sc, rc, sd, rd, sroute, rroute, srx, rrx,
):
    nz = n_expert // 2
    last = nz - 1
    count, width = x_ref.shape
    half = count // 2
    shares = g.shape[1]
    e, h, z, core, x, y, across_x, across_y, sibling = places()
    hx, hy, hd = across_x[1], across_y[1], (1 - y) * 2 + (1 - x)
    load = [
        pltpu.make_async_copy(src, w.at[i], w_sem.at[i])
        for i, src in enumerate((wg_hbm, wu_hbm, wd_hbm))
    ]
    for copy in load:
        copy.start()
    top = ids_ref.shape[0]
    meta_ref[:top] = ids_ref[...].astype(F32)
    meta_ref[top:] = rw_ref[...]
    greet(n_expert, e, h, across_x, across_y)
    full = (x_ref, dy_ref)

    def block(t, b, share, start=0, size=count):
        return g.at[t, share, pl.ds(pl.multiple_of(b * count + start, 32), size)]

    own = [pltpu.make_async_copy(full[t], block(t, e, h), own_sem.at[t]) for t in range(2)]
    own.append(pltpu.make_async_copy(meta_ref, gm.at[e], own_sem.at[2]))

    def arrived(slot, send_sem, recv_sem, device):
        send(slot, slot, send_sem, recv_sem, device).wait_recv()

    def meta_to(i):
        return send(meta_ref, gm.at[e], ms.at[i], mr.at[i], ((e + n_expert - i) % n_expert, h))

    def apart(j):
        return j + (j // 2) * (5 - 2 * j)

    def plane_of(j):
        return flip(z, apart(j))

    def column(j):
        return plane_of(j) * 2 + core

    def z_send(t, j):
        i = apart(j)
        return send(full[t], block(t, e, h), zs.at[t, i], zr.at[t, i], (column(j), h))

    def first_sends(t, j, src):
        slot = block(t, column(j), h)
        src = slot if src is None else src
        return [
            send(src, slot, xsem.at[t, j], xr.at[t, j], across_x),
            send(src, slot, ysem.at[t, j], yr.at[t, j], across_y),
            send(src, slot, ss.at[t, j, 0], sr.at[t, j, 0], sibling),
        ]

    def second_sends(t, j, side):
        share, to = ((hx, across_y), (hy, across_x))[side]
        slot = block(t, column(j), share)
        part = block(t, column(j), share, side * half, half)
        return [
            send(part, part, ds.at[t, j, side], dr.at[t, j, side], to),
            send(slot, slot, ss.at[t, j, 1 + side], sr.at[t, j, 1 + side], sibling),
        ]

    def third_sends(t, j):
        slot = block(t, column(j), hd)
        return [send(slot, slot, ss.at[t, j, 3], sr.at[t, j, 3], sibling)]

    def start(copies):
        for copy in copies:
            copy.start()

    def sent(copies):
        for copy in copies:
            copy.wait_send()

    def first(t, j):
        i = apart(j)
        arrived(block(t, column(j), h), zs.at[t, i], zr.at[t, i], across_x)
        start(first_sends(t, j, None))

    def second(t, j):
        arrived(block(t, column(j), hx), xsem.at[t, j], xr.at[t, j], across_x)
        start(second_sends(t, j, 0))
        arrived(block(t, column(j), hy), ysem.at[t, j], yr.at[t, j], across_y)
        start(second_sends(t, j, 1))

    def third(t, j):
        for k in range(2):
            arrived(block(t, column(j), hd, k * half, half), ds.at[t, j, k], dr.at[t, j, k], across_y)
        start(third_sends(t, j))

    def from_sibling(t, j):
        b = plane_of(j) * 2 + (1 - core)
        for k, part in enumerate((h, hx, hy, hd)):
            arrived(block(t, b, part), ss.at[t, j, k], sr.at[t, j, k], sibling)

    start(first_sends(0, 0, x_ref))
    start([meta_to(i) for i in range(1, n_expert)])
    z_send(0, 1).start()
    start(first_sends(1, 0, dy_ref))
    z_send(1, 1).start()
    for j in range(2, nz):
        for t in range(2):
            z_send(t, j).start()
    start(own)
    second(0, 0)
    first(0, 1)
    second(1, 0)
    first(1, 1)
    third(0, 0)
    for copy in load + own:
        copy.wait()
    for i in range(1, n_expert):
        arrived(gm.at[(e + i) % n_expert], ms.at[i], mr.at[i], sibling)

    turned = (((1,), (1,)), ((), ()))
    low, high = pl.ds(0, half), pl.ds(half, half)

    def add(a, b):
        return (a.astype(F32) + b.astype(F32)).astype(BF16)

    def a_send(j, s):
        return send(tok.at[1 - core, s], got_a.at[j, s], sa.at[j, s], ra.at[j, s], sibling)

    def b_sends(j):
        return [
            send(got_a.at[j, k * 2 + (1 - x), low], got_bx.at[j, k], sbx.at[j, k], rbx.at[j, k], across_x)
            for k in (1 - y, y)
        ] + [
            send(got_a.at[j, (1 - y) * 2 + k, high], got_by.at[j, k], sby.at[j, k], rby.at[j, k], across_y)
            for k in (1 - x, x)
        ]

    def c_sends(j):
        return [
            send(got_bx.at[j, 1 - y], got_c.at[j, low], sc.at[j, 0], rc.at[j, 0], across_y),
            send(got_by.at[j, 1 - x], got_c.at[j, high], sc.at[j, 1], rc.at[j, 1], across_x),
        ]

    def d_send(j):
        i = apart(j)
        return send(got_c.at[j], got_d.at[i], sd.at[i], rd.at[i], (column(j), h))

    def fold(j):
        for s in range(shares):
            a_send(j, s).wait()
            got_a[j, s] = add(tok[core, s], got_a[j, s])

    def stage_b(j):
        start(b_sends(j))

    def stage_c(j):
        near_x, near_y = b_sends(j)[0::2]
        onward = c_sends(j)
        near_x.wait_recv()
        got_bx[j, 1 - y] = add(got_a[j, (1 - y) * 2 + x, low], got_bx[j, 1 - y])
        onward[0].start()
        near_y.wait_recv()
        got_by[j, 1 - x] = add(got_a[j, y * 2 + (1 - x), high], got_by[j, 1 - x])
        onward[1].start()

    def stage_d(j):
        for copy in b_sends(j)[1::2]:
            copy.wait_recv()
        got_bx[j, y] = add(got_a[j, h, low], got_bx[j, y])
        got_by[j, x] = add(got_a[j, h, high], got_by[j, x])
        for copy in c_sends(j):
            copy.wait_recv()
        got_c[j, low] = add(got_bx[j, y], got_c[j, low])
        got_c[j, high] = add(got_by[j, x], got_c[j, high])
        if j:
            d_send(j).start()

    rx = send(route, route_x, srx.at[0], rrx.at[0], across_x)
    ry = send(route_s, route_y, srx.at[1], rrx.at[1], across_y)
    routes = [
        send(route_t.at[(e + i) % n_expert], route_z.at[i], sroute.at[i], rroute.at[i], ((e + i) % n_expert, h))
        for i in range(1, n_expert)
    ]

    def at_share(s):
        return pl.ds(s * width, width)

    def project(t, rows, m):
        total = None
        for s in range(shares):
            part = lax.dot_general(
                g[t, s, rows], w[m, :, at_share(s)], turned, preferred_element_type=F32
            )
            total = part if total is None else total + part
        return total

    eye = diagonal(count)

    def step(j, carry):
        more, further, final = j + 1 < nz, j + 2 < nz, j == last
        plane = plane_of(j)
        rows = pl.ds(pl.multiple_of(plane * (2 * count), 64), 2 * count)
        from_sibling(0, j)

        @pl.when(more)
        def _():
            second(0, j + 1)

        gate = project(0, rows, 0)
        up = project(0, rows, 1)

        @pl.when(further)
        def _():
            first(0, j + 2)

        @pl.when(j > 0)
        def _():
            fold(j - 1)

        @pl.when(final)
        def _():
            stage_b(last - 1)

        third(1, j)
        from_sibling(1, j)
        back = project(1, rows, 2)
        hits, weights = [], []
        for c in range(2):
            hit, row = routed(gm[plane * 2 + c], e)
            hits.append(hit)
            weights.append(jnp.sum(eye * row, axis=1, keepdims=True))
        weight = jnp.concatenate(weights, axis=0)
        sig = jax.nn.sigmoid(gate)
        act = gate * sig
        hidden = act * up
        d[2, rows] = (weight * hidden).astype(BF16)
        hidden = hidden.astype(BF16)
        parted = jnp.sum(hidden.astype(F32) * back, axis=1, keepdims=True)
        grad_hidden = weight * back
        d[0, rows] = (grad_hidden * up * sig * (1.0 + gate * (1.0 - sig))).astype(BF16)
        d[1, rows] = (grad_hidden * act).astype(BF16)
        for c in range(2):
            per_token = jnp.sum(eye * parted[c * count : (c + 1) * count], axis=0, keepdims=True)
            route[plane * 2 + c, :top] = hits[c] * per_token
            route[plane * 2 + c, top:] = jnp.zeros_like(hits[c])

        @pl.when(more)
        def _():
            second(1, j + 1)

        @pl.when(further)
        def _():
            first(1, j + 2)

        @pl.when(j == last - 1)
        def _():
            stage_b(1)

        @pl.when(more)
        def _():
            third(0, j + 1)

        @pl.when(final)
        def _():
            rx.start()
            stage_c(1)

        for s in range(shares):
            row_grad = (
                jnp.dot(d[0, rows], w[0, :, at_share(s)], preferred_element_type=F32)
                + jnp.dot(d[1, rows], w[1, :, at_share(s)], preferred_element_type=F32)
            ).astype(BF16)
            for c in range(2):
                tok[c, s] = row_grad[c * count : (c + 1) * count]
            if s == 1:

                @pl.when(final)
                def _():
                    stage_c(last - 1)

        for s in range(shares):
            a_send(j, s).start()
        return carry

    lax.fori_loop(0, nz, step, 0)

    def route_on():
        rx.wait_recv()
        route_s[...] = route[...] + route_x[...]
        ry.start()

    def route_out_to_owners():
        ry.wait_recv()
        route_t[...] = route_s[...] + route_y[...]
        start(routes)

    def last_rows():
        fold(last)
        stage_b(last)
        route_on()

    def one_plane():
        stage_d(1)
        stage_b(0)

    def two_planes():
        stage_d(last - 1)
        route_out_to_owners()

    events = {
        (0, 0): last_rows,
        (0, 1): one_plane,
        (0, 2): two_planes,
        (0, 3): lambda: stage_c(last),
        (1, 1): lambda: stage_d(last),
        (1, 2): lambda: stage_c(0),
        (2, 0): lambda: stage_d(0),
    }

    def outer(m, carry):
        for s in range(shares):
            w[m, :, at_share(s)] = lax.dot_general(
                d[m], g[m // 2, s], (((0,), (0,)), ((), ())), preferred_element_type=F32
            ).astype(BF16)
            for (at_m, at_s), event in events.items():
                if at_s == s:
                    pl.when(m == at_m)(event)
        return carry

    lax.fori_loop(0, 3, outer, 0)
    total = route_t[e]
    for i in range(1, n_expert):
        routes[i - 1].wait_recv()
        total = total + route_z[i]
    route_out[...] = total[:top]
    total = got_c[0].astype(F32)
    for j in range(1, nz):
        d_send(j).wait_recv()
        total = total + got_d[apart(j)].astype(F32)
    grad_out[...] = total.astype(BF16)
    sent([rx, ry] + routes + [d_send(j) for j in range(1, nz)])
    for j in range(nz):
        sent(b_sends(j) + c_sends(j))
    for i in range(1, n_expert):
        meta_to(i).wait_send()
    for t in range(2):
        for j in range(nz):
            if j:
                z_send(t, j).wait_send()
            sent(first_sends(t, j, full[t] if j == 0 else None))
            sent(second_sends(t, j, 0) + second_sends(t, j, 1) + third_sends(t, j))


def gather_and_expert(x, dy, ids, route_weight, w_gate, w_up, w_down, n_expert):
    nz = n_expert // 2
    top = ids.shape[0]
    meta = (2 * top, ids.shape[1])
    count, width = x.shape
    hidden, depth = w_gate.shape
    total = n_expert * count
    half = count // 2
    dma = pltpu.SemaphoreType.DMA
    vmem = pl.BlockSpec(memory_space=pltpu.VMEM)
    hbm = pl.BlockSpec(memory_space=pl.ANY)

    def room(*shape):
        return pltpu.VMEM(shape, BF16)

    return pl.pallas_call(
        functools.partial(fused_kernel, n_expert),
        out_shape=(
            room(3, hidden, depth),
            jax.ShapeDtypeStruct((count, width), BF16),
            jax.ShapeDtypeStruct(ids.shape, F32),
        ),
        in_specs=[vmem] * 4 + [hbm] * 3,
        out_specs=[vmem] * 3,
        scratch_shapes=[
            room(2, 4, total, width),
            pltpu.VMEM(meta, F32),
            pltpu.VMEM((n_expert,) + meta, F32),
            room(3, total, hidden),
            room(2, 4, count, width),
            room(nz, 4, count, width),
            room(nz, 2, half, width),
            room(nz, 2, half, width),
            room(nz, count, width),
            room(nz, count, width),
        ]
        + [pltpu.VMEM((n_expert,) + meta, F32)] * 6
        + [dma((3,))]
        + [dma((2, nz))] * 6
        + [dma((2, nz, 2))] * 2
        + [dma((2, nz, 4))] * 2
        + [dma((n_expert,))] * 2
        + [dma((3,))]
        + [dma((nz, 4))] * 2
        + [dma((nz, 2))] * 6
        + [dma((nz,))] * 2
        + [dma((n_expert,))] * 2
        + [dma((2,))] * 2,
        compiler_params=pltpu.CompilerParams(
            collective_id=0, has_side_effects=True, vmem_limit_bytes=50 * 1024 * 1024
        ),
    )(x, dy, ids, route_weight, w_gate, w_up, w_down)


def paired_device(inputs, out_grad, expert_ids, route_weight, w_gate, w_up, w_down):
    grads, grad_input, grad_route = gather_and_expert(
        inputs, out_grad, expert_ids.T, route_weight.T, w_gate[0], w_up[0], w_down[0], lax.axis_size("expert")
    )
    wide = [grads[i].astype(F32)[None] for i in range(3)]
    return (grad_input, grad_route.T, *wide)


def solution(mesh):
    placed = (
        P("expert", "hidden"),
        P("expert", "hidden"),
        P("expert", None),
        P("expert", None),
        P("expert", "hidden", None),
        P("expert", "hidden", None),
        P("expert", "hidden", None),
    )
    return jax.shard_map(
        paired_device
        if mesh.shape["hidden"] == 4 and mesh.shape["expert"] == 8
        else plain_device,
        mesh=mesh,
        in_specs=placed,
        out_specs=(
            P("expert", "hidden"),
            P("expert", None),
            P("expert", "hidden", None),
            P("expert", "hidden", None),
            P("expert", "hidden", None),
        ),
        check_vma=False,
    )
```

```python
import functools

import jax
import jax.numpy as jnp
from jax import lax
from jax.experimental import pallas as pl
from jax.experimental.pallas import tpu as pltpu
from jax.sharding import PartitionSpec as P


def slot_tables(expert_ids, experts, capacity):
    count, top = expert_ids.shape
    flat = expert_ids.reshape(-1)
    onehot = (flat[:, None] == jnp.arange(experts, dtype=jnp.int32)[None, :]).astype(jnp.int32)
    position = jnp.cumsum(onehot, axis=0) - 1
    slot = jnp.sum(onehot * position, axis=1)
    dest = flat * capacity + slot
    table = (
        jnp.zeros((experts * capacity,), jnp.int32)
        .at[dest]
        .set(jnp.arange(count * top, dtype=jnp.int32))
    )
    filled = jnp.zeros((experts * capacity,), jnp.int32).at[dest].set(1)
    return (dest, table, filled)


def pack_rows(values, table, filled, top, experts, capacity):
    picked = values[table // top] * filled.astype(values.dtype)[:, None]
    return picked.reshape(experts, capacity, values.shape[1])


def to_local(buffer, n_groups, local_count):
    rest = buffer.shape[2:]
    shaped = buffer.reshape((n_groups, local_count, buffer.shape[1]) + rest)
    return jnp.swapaxes(shaped, 0, 1).reshape((local_count, n_groups * buffer.shape[1]) + rest)


def from_local(buffer, n_groups, capacity):
    local_count = buffer.shape[0]
    rest = buffer.shape[2:]
    shaped = buffer.reshape((local_count, n_groups, capacity) + rest)
    return jnp.swapaxes(shaped, 0, 1).reshape((n_groups * local_count, capacity) + rest)


def plain_device(inputs, out_grad, expert_ids, route_weight, w_gate, w_up, w_down):
    n_groups = lax.axis_size("expert")
    local_count = w_gate.shape[0]
    experts = local_count * n_groups
    tok_count, top = expert_ids.shape
    capacity = 3 * top * tok_count // (2 * experts)
    dest, table, filled = slot_tables(expert_ids, experts, capacity)
    send_weight = (route_weight.reshape(-1)[table] * filled.astype(jnp.float32)).reshape(
        experts, capacity
    )
    send_x = pack_rows(inputs, table, filled, top, experts, capacity)
    send_dy = pack_rows(out_grad, table, filled, top, experts, capacity)
    got_x, got_dy, got_weight = (
        lax.all_to_all(send_x, "expert", split_axis=0, concat_axis=0, tiled=True),
        lax.all_to_all(send_dy, "expert", split_axis=0, concat_axis=0, tiled=True),
        lax.all_to_all(
            send_weight.astype(jnp.bfloat16), "expert", split_axis=0, concat_axis=0, tiled=True
        ).astype(send_weight.dtype),
    )
    rows_x, rows_dy = (
        lax.all_gather(got_x, "hidden", axis=2, tiled=True),
        lax.all_gather(got_dy, "hidden", axis=2, tiled=True),
    )
    xs = to_local(rows_x, n_groups, local_count)
    dys = to_local(rows_dy, n_groups, local_count)
    weights = to_local(got_weight, n_groups, local_count)
    gate = jnp.einsum("esd,efd->esf", xs, w_gate, preferred_element_type=jnp.float32)
    up = jnp.einsum("esd,efd->esf", xs, w_up, preferred_element_type=jnp.float32)
    sig = jax.nn.sigmoid(gate)
    act = gate * sig
    hidden = (act * up).astype(jnp.bfloat16)
    back = jnp.einsum("esd,efd->esf", dys, w_down, preferred_element_type=jnp.float32)
    route_part = jnp.sum(hidden.astype(jnp.float32) * back, axis=2)
    grad_hidden = weights[:, :, None] * back
    scaled = (weights[:, :, None] * dys.astype(jnp.float32)).astype(jnp.bfloat16)
    grad_down = jnp.einsum("esf,esd->efd", hidden, scaled, preferred_element_type=jnp.float32)
    d_gate = (grad_hidden * up * sig * (1.0 + gate * (1.0 - sig))).astype(jnp.bfloat16)
    d_up = (grad_hidden * act).astype(jnp.bfloat16)
    grad_gate = jnp.einsum("esf,esd->efd", d_gate, xs, preferred_element_type=jnp.float32)
    grad_up = jnp.einsum("esf,esd->efd", d_up, xs, preferred_element_type=jnp.float32)
    partial_value = jnp.einsum("esf,efd->esd", d_gate, w_gate, preferred_element_type=jnp.float32)
    partial_value = partial_value + jnp.einsum(
        "esf,efd->esd", d_up, w_up, preferred_element_type=jnp.float32
    )
    route_total = lax.psum(route_part, "hidden")
    route_back = from_local(route_total, n_groups, capacity)
    summed = lax.psum_scatter(
        partial_value.astype(jnp.bfloat16), "hidden", scatter_dimension=2, tiled=True
    ).astype(jnp.float32)
    back_rows, back_route = (
        lax.all_to_all(
            from_local(summed, n_groups, capacity).astype(jnp.bfloat16),
            "expert",
            split_axis=0,
            concat_axis=0,
            tiled=True,
        ).astype(jnp.float32),
        lax.all_to_all(
            route_back.astype(jnp.bfloat16), "expert", split_axis=0, concat_axis=0, tiled=True
        ).astype(route_back.dtype),
    )
    per_pair = back_rows.reshape(experts * capacity, back_rows.shape[2])[dest]
    grad_input = jnp.sum(per_pair.reshape(tok_count, top, per_pair.shape[1]), axis=1).astype(
        jnp.bfloat16
    )
    grad_route = back_route.reshape(-1)[dest].reshape(tok_count, top)
    return (grad_input, grad_route, grad_gate, grad_up, grad_down)


MESH = pl.DeviceIdType.MESH
F32 = jnp.float32
BF16 = jnp.bfloat16


def places():
    e, h = lax.axis_index("expert"), lax.axis_index("hidden")
    core, z = e % 2, e // 2
    x, y = h % 2, h // 2
    across_x = (e, y * 2 + (1 - x))
    across_y = (e, (1 - y) * 2 + x)
    sibling = (z * 2 + (1 - core), h)
    return e, h, z, core, x, y, across_x, across_y, sibling


def flip(z, j):
    low = z % 2 + j % 2 - 2 * (z % 2) * (j % 2)
    high = z // 2 + j // 2 - 2 * (z // 2) * (j // 2)
    return low + 2 * high


def greet(n_expert, e, h, across_x, across_y):
    barrier = pltpu.get_barrier_semaphore()
    peers = [((e + i) % n_expert, h) for i in range(1, n_expert)] + [across_x, across_y]
    for peer in peers:
        pl.semaphore_signal(barrier, inc=1, device_id=peer, device_id_type=MESH)
    pl.semaphore_wait(barrier, len(peers))


def send(src, dst, send_sem, recv_sem, device):
    return pltpu.make_async_remote_copy(
        src_ref=src, dst_ref=dst, send_sem=send_sem, recv_sem=recv_sem,
        device_id=device, device_id_type=MESH,
    )


def routed(meta, e):
    top = meta.shape[0] // 2
    hits = (meta[:top] == e.astype(F32)).astype(F32)
    return hits, jnp.sum(hits * meta[top:], axis=0, keepdims=True)


def diagonal(count):
    return (
        lax.broadcasted_iota(jnp.int32, (count, count), 0)
        == lax.broadcasted_iota(jnp.int32, (count, count), 1)
    ).astype(F32)


def fused_kernel(
    n_expert, x_ref, dy_ref, ids_ref, rw_ref, wg_hbm, wu_hbm, wd_hbm,
    w, grad_out, route_out,
    g, meta_ref, gm, d, tok, got_a, got_bx, got_by, got_c, got_d,
    route, route_x, route_s, route_y, route_t, route_z,
    own_sem, zs, zr, xsem, xr, ysem, yr, ds, dr, ss, sr, ms, mr, w_sem,
    sa, ra, sbx, rbx, sby, rby, sc, rc, sd, rd, sroute, rroute, srx, rrx,
):
    nz = n_expert // 2
    last = nz - 1
    count, width = x_ref.shape
    half = count // 2
    shares = g.shape[1]
    e, h, z, core, x, y, across_x, across_y, sibling = places()
    hx, hy, hd = across_x[1], across_y[1], (1 - y) * 2 + (1 - x)
    load = [
        pltpu.make_async_copy(src, w.at[i], w_sem.at[i])
        for i, src in enumerate((wg_hbm, wu_hbm, wd_hbm))
    ]
    for copy in load:
        copy.start()
    top = ids_ref.shape[0]
    meta_ref[:top] = ids_ref[...].astype(F32)
    meta_ref[top:] = rw_ref[...]
    greet(n_expert, e, h, across_x, across_y)
    full = (x_ref, dy_ref)

    def block(t, b, share, start=0, size=count):
        return g.at[t, share, pl.ds(pl.multiple_of(b * count + start, 32), size)]

    own = [pltpu.make_async_copy(full[t], block(t, e, h), own_sem.at[t]) for t in range(2)]
    own.append(pltpu.make_async_copy(meta_ref, gm.at[e], own_sem.at[2]))

    def arrived(slot, send_sem, recv_sem, device):
        send(slot, slot, send_sem, recv_sem, device).wait_recv()

    def meta_to(i):
        return send(meta_ref, gm.at[e], ms.at[i], mr.at[i], ((e + n_expert - i) % n_expert, h))

    def apart(j):
        return j + (j // 2) * (5 - 2 * j)

    def plane_of(j):
        return flip(z, apart(j))

    def column(j):
        return plane_of(j) * 2 + core

    def z_send(t, j):
        i = apart(j)
        return send(full[t], block(t, e, h), zs.at[t, i], zr.at[t, i], (column(j), h))

    def first_sends(t, j, src):
        slot = block(t, column(j), h)
        src = slot if src is None else src
        return [
            send(src, slot, xsem.at[t, j], xr.at[t, j], across_x),
            send(src, slot, ysem.at[t, j], yr.at[t, j], across_y),
            send(src, slot, ss.at[t, j, 0], sr.at[t, j, 0], sibling),
        ]

    def second_sends(t, j, side):
        share, to = ((hx, across_y), (hy, across_x))[side]
        slot = block(t, column(j), share)
        part = block(t, column(j), share, side * half, half)
        return [
            send(part, part, ds.at[t, j, side], dr.at[t, j, side], to),
            send(slot, slot, ss.at[t, j, 1 + side], sr.at[t, j, 1 + side], sibling),
        ]

    def third_sends(t, j):
        slot = block(t, column(j), hd)
        return [send(slot, slot, ss.at[t, j, 3], sr.at[t, j, 3], sibling)]

    def start(copies):
        for copy in copies:
            copy.start()

    def sent(copies):
        for copy in copies:
            copy.wait_send()

    def first(t, j):
        i = apart(j)
        arrived(block(t, column(j), h), zs.at[t, i], zr.at[t, i], across_x)
        start(first_sends(t, j, None))

    def second(t, j):
        arrived(block(t, column(j), hx), xsem.at[t, j], xr.at[t, j], across_x)
        start(second_sends(t, j, 0))
        arrived(block(t, column(j), hy), ysem.at[t, j], yr.at[t, j], across_y)
        start(second_sends(t, j, 1))

    def third(t, j):
        for k in range(2):
            arrived(block(t, column(j), hd, k * half, half), ds.at[t, j, k], dr.at[t, j, k], across_y)
        start(third_sends(t, j))

    def from_sibling(t, j):
        b = plane_of(j) * 2 + (1 - core)
        for k, part in enumerate((h, hx, hy, hd)):
            arrived(block(t, b, part), ss.at[t, j, k], sr.at[t, j, k], sibling)

    start(first_sends(0, 0, x_ref))
    start([meta_to(i) for i in range(1, n_expert)])
    z_send(0, 1).start()
    start(first_sends(1, 0, dy_ref))
    z_send(1, 1).start()
    for j in range(2, nz):
        for t in range(2):
            z_send(t, j).start()
    start(own)
    second(0, 0)
    first(0, 1)
    second(1, 0)
    first(1, 1)
    third(0, 0)
    for copy in load + own:
        copy.wait()
    for i in range(1, n_expert):
        arrived(gm.at[(e + i) % n_expert], ms.at[i], mr.at[i], sibling)

    turned = (((1,), (1,)), ((), ()))
    low, high = pl.ds(0, half), pl.ds(half, half)

    def add(a, b):
        return (a.astype(F32) + b.astype(F32)).astype(BF16)

    def a_send(j, s):
        return send(tok.at[1 - core, s], got_a.at[j, s], sa.at[j, s], ra.at[j, s], sibling)

    def b_sends(j):
        return [
            send(got_a.at[j, k * 2 + (1 - x), low], got_bx.at[j, k], sbx.at[j, k], rbx.at[j, k], across_x)
            for k in (1 - y, y)
        ] + [
            send(got_a.at[j, (1 - y) * 2 + k, high], got_by.at[j, k], sby.at[j, k], rby.at[j, k], across_y)
            for k in (1 - x, x)
        ]

    def c_sends(j):
        return [
            send(got_bx.at[j, 1 - y], got_c.at[j, low], sc.at[j, 0], rc.at[j, 0], across_y),
            send(got_by.at[j, 1 - x], got_c.at[j, high], sc.at[j, 1], rc.at[j, 1], across_x),
        ]

    def d_send(j):
        i = apart(j)
        return send(got_c.at[j], got_d.at[i], sd.at[i], rd.at[i], (column(j), h))

    def fold(j):
        for s in range(shares):
            a_send(j, s).wait()
            got_a[j, s] = add(tok[core, s], got_a[j, s])

    def stage_b(j):
        start(b_sends(j))

    def stage_c(j):
        near_x, near_y = b_sends(j)[0::2]
        onward = c_sends(j)
        near_x.wait_recv()
        got_bx[j, 1 - y] = add(got_a[j, (1 - y) * 2 + x, low], got_bx[j, 1 - y])
        onward[0].start()
        near_y.wait_recv()
        got_by[j, 1 - x] = add(got_a[j, y * 2 + (1 - x), high], got_by[j, 1 - x])
        onward[1].start()

    def stage_d(j):
        for copy in b_sends(j)[1::2]:
            copy.wait_recv()
        got_bx[j, y] = add(got_a[j, h, low], got_bx[j, y])
        got_by[j, x] = add(got_a[j, h, high], got_by[j, x])
        for copy in c_sends(j):
            copy.wait_recv()
        got_c[j, low] = add(got_bx[j, y], got_c[j, low])
        got_c[j, high] = add(got_by[j, x], got_c[j, high])
        if j:
            d_send(j).start()

    rx = send(route, route_x, srx.at[0], rrx.at[0], across_x)
    ry = send(route_s, route_y, srx.at[1], rrx.at[1], across_y)
    routes = [
        send(route_t.at[(e + i) % n_expert], route_z.at[i], sroute.at[i], rroute.at[i], ((e + i) % n_expert, h))
        for i in range(1, n_expert)
    ]

    def at_share(s):
        return pl.ds(s * width, width)

    def project(t, rows, m):
        total = None
        for s in range(shares):
            part = lax.dot_general(
                g[t, s, rows], w[m, :, at_share(s)], turned, preferred_element_type=F32
            )
            total = part if total is None else total + part
        return total

    eye = diagonal(count)

    def step(j, carry):
        more, further, final = j + 1 < nz, j + 2 < nz, j == last
        plane = plane_of(j)
        rows = pl.ds(pl.multiple_of(plane * (2 * count), 64), 2 * count)
        from_sibling(0, j)

        @pl.when(more)
        def _():
            second(0, j + 1)

        gate = project(0, rows, 0)
        up = project(0, rows, 1)

        @pl.when(further)
        def _():
            first(0, j + 2)

        @pl.when(j > 0)
        def _():
            fold(j - 1)

        @pl.when(final)
        def _():
            stage_b(last - 1)

        third(1, j)
        from_sibling(1, j)
        back = project(1, rows, 2)
        hits, weights = [], []
        for c in range(2):
            hit, row = routed(gm[plane * 2 + c], e)
            hits.append(hit)
            weights.append(jnp.sum(eye * row, axis=1, keepdims=True))
        weight = jnp.concatenate(weights, axis=0)
        sig = jax.nn.sigmoid(gate)
        act = gate * sig
        hidden = act * up
        d[2, rows] = (weight * hidden).astype(BF16)
        hidden = hidden.astype(BF16)
        parted = jnp.sum(hidden.astype(F32) * back, axis=1, keepdims=True)
        grad_hidden = weight * back
        d[0, rows] = (grad_hidden * up * sig * (1.0 + gate * (1.0 - sig))).astype(BF16)
        d[1, rows] = (grad_hidden * act).astype(BF16)
        for c in range(2):
            per_token = jnp.sum(eye * parted[c * count : (c + 1) * count], axis=0, keepdims=True)
            route[plane * 2 + c, :top] = hits[c] * per_token
            route[plane * 2 + c, top:] = jnp.zeros_like(hits[c])

        @pl.when(more)
        def _():
            second(1, j + 1)

        @pl.when(further)
        def _():
            first(1, j + 2)

        @pl.when(j == last - 1)
        def _():
            stage_b(1)

        @pl.when(more)
        def _():
            third(0, j + 1)

        @pl.when(final)
        def _():
            rx.start()
            stage_c(1)

        for s in range(shares):
            row_grad = (
                jnp.dot(d[0, rows], w[0, :, at_share(s)], preferred_element_type=F32)
                + jnp.dot(d[1, rows], w[1, :, at_share(s)], preferred_element_type=F32)
            ).astype(BF16)
            for c in range(2):
                tok[c, s] = row_grad[c * count : (c + 1) * count]
        for s in range(shares):
            a_send(j, s).start()
        return carry

    lax.fori_loop(0, nz, step, 0)

    def route_on():
        rx.wait_recv()
        route_s[...] = route[...] + route_x[...]
        ry.start()

    def route_out_to_owners():
        ry.wait_recv()
        route_t[...] = route_s[...] + route_y[...]
        start(routes)

    def last_rows():
        fold(last)
        stage_b(last)
        stage_d(1)
        route_on()

    def last_on():
        stage_c(last)
        stage_b(0)

    def two_planes():
        stage_d(last - 1)
        route_out_to_owners()

    events = {
        (0, 0): last_rows,
        (0, 1): two_planes,
        (0, 3): last_on,
        (1, 1): lambda: stage_d(last),
        (1, 3): lambda: stage_c(0),
        (2, 1): lambda: stage_d(0),
    }

    def outer(m, carry):
        for s in range(shares):
            w[m, :, at_share(s)] = lax.dot_general(
                d[m], g[m // 2, s], (((0,), (0,)), ((), ())), preferred_element_type=F32
            ).astype(BF16)
            for (at_m, at_s), event in events.items():
                if at_s == s:
                    pl.when(m == at_m)(event)
        return carry

    stage_c(last - 1)
    lax.fori_loop(0, 3, outer, 0)
    total = route_t[e]
    for i in range(1, n_expert):
        routes[i - 1].wait_recv()
        total = total + route_z[i]
    route_out[...] = total[:top]
    total = got_c[0].astype(F32)
    for j in range(1, nz):
        d_send(j).wait_recv()
        total = total + got_d[apart(j)].astype(F32)
    grad_out[...] = total.astype(BF16)
    sent([rx, ry] + routes + [d_send(j) for j in range(1, nz)])
    for j in range(nz):
        sent(b_sends(j) + c_sends(j))
    for i in range(1, n_expert):
        meta_to(i).wait_send()
    for t in range(2):
        for j in range(nz):
            if j:
                z_send(t, j).wait_send()
            sent(first_sends(t, j, full[t] if j == 0 else None))
            sent(second_sends(t, j, 0) + second_sends(t, j, 1) + third_sends(t, j))


def gather_and_expert(x, dy, ids, route_weight, w_gate, w_up, w_down, n_expert):
    nz = n_expert // 2
    top = ids.shape[0]
    meta = (2 * top, ids.shape[1])
    count, width = x.shape
    hidden, depth = w_gate.shape
    total = n_expert * count
    half = count // 2
    dma = pltpu.SemaphoreType.DMA
    vmem = pl.BlockSpec(memory_space=pltpu.VMEM)
    hbm = pl.BlockSpec(memory_space=pl.ANY)

    def room(*shape):
        return pltpu.VMEM(shape, BF16)

    return pl.pallas_call(
        functools.partial(fused_kernel, n_expert),
        out_shape=(
            room(3, hidden, depth),
            jax.ShapeDtypeStruct((count, width), BF16),
            jax.ShapeDtypeStruct(ids.shape, F32),
        ),
        in_specs=[vmem] * 4 + [hbm] * 3,
        out_specs=[vmem] * 3,
        scratch_shapes=[
            room(2, 4, total, width),
            pltpu.VMEM(meta, F32),
            pltpu.VMEM((n_expert,) + meta, F32),
            room(3, total, hidden),
            room(2, 4, count, width),
            room(nz, 4, count, width),
            room(nz, 2, half, width),
            room(nz, 2, half, width),
            room(nz, count, width),
            room(nz, count, width),
        ]
        + [pltpu.VMEM((n_expert,) + meta, F32)] * 6
        + [dma((3,))]
        + [dma((2, nz))] * 6
        + [dma((2, nz, 2))] * 2
        + [dma((2, nz, 4))] * 2
        + [dma((n_expert,))] * 2
        + [dma((3,))]
        + [dma((nz, 4))] * 2
        + [dma((nz, 2))] * 6
        + [dma((nz,))] * 2
        + [dma((n_expert,))] * 2
        + [dma((2,))] * 2,
        compiler_params=pltpu.CompilerParams(
            collective_id=0, has_side_effects=True, vmem_limit_bytes=50 * 1024 * 1024
        ),
    )(x, dy, ids, route_weight, w_gate, w_up, w_down)


def paired_device(inputs, out_grad, expert_ids, route_weight, w_gate, w_up, w_down):
    grads, grad_input, grad_route = gather_and_expert(
        inputs, out_grad, expert_ids.T, route_weight.T, w_gate[0], w_up[0], w_down[0], lax.axis_size("expert")
    )
    wide = [grads[i].astype(F32)[None] for i in range(3)]
    return (grad_input, grad_route.T, *wide)


def solution(mesh):
    placed = (
        P("expert", "hidden"),
        P("expert", "hidden"),
        P("expert", None),
        P("expert", None),
        P("expert", "hidden", None),
        P("expert", "hidden", None),
        P("expert", "hidden", None),
    )
    return jax.shard_map(
        paired_device
        if mesh.shape["hidden"] == 4 and mesh.shape["expert"] == 8
        else plain_device,
        mesh=mesh,
        in_specs=placed,
        out_specs=(
            P("expert", "hidden"),
            P("expert", None),
            P("expert", "hidden", None),
            P("expert", "hidden", None),
            P("expert", "hidden", None),
        ),
        check_vma=False,
    )
```
